32 devices in a mesh: row: 4 (over z), col: 2 (over y), dp: 4 (over x, core).
Axes of the slice: x: 2, y: 2, z: 4, core: 2. Of those that a mesh axis runs over, the one named last changes fastest.
Arguments:
- inputs: bfloat16 [4096, 4096], P('dp', 'row'), may hold values from -6 to 6
- upstream: bfloat16 [4096, 4096], P('dp', 'row'), may hold values from -6 to 6
- expand: bfloat16 [4096, 16384], P('row', 'col'), may hold values from -0.09375 to 0.09375
- biases: float32 [16384], P('col'), may hold values from -5 to 5
- contract: bfloat16 [16384, 4096], P('col', 'row'), may hold values from -0.046875 to 0.046875
Outputs:
- grad_inputs: bfloat16 [4096, 4096], P('dp', 'row')
- grad_expand: bfloat16 [4096, 16384], P('row', 'col')
- grad_biases: bfloat16 [16384], P('col')
- grad_contract: bfloat16 [16384, 4096], P('col', 'row')
- grad_offset: bfloat16 [4096], P('row')
The draws below stay inside these ranges and needn't reach their ends.
All inputs are finite; a program needn't handle non-finite values.
Results may differ from the reference program's by a relative error of at most 0.022.
Values may be sent and summed in bfloat16 or wider, within the bound.
No kernel may reach another device: no remote copies, remote signals or barrier semaphores. Data moves between devices by JAX's collectives and lax.ppermute only.
A program may use at most 192 MiB of HBM per device.

```python
import jax
import jax.numpy as jnp
from jax import lax

D = 4096
FF = 16384
TOK_DEV = 1024
TOKENS = 4096
N_ROW = 4
N_COL = 2
N_DP = 4


def levels(rng, extent, pieces, least, largest):
    level = 1.0
    for dim, parts in pieces:
        heights = jax.random.uniform(jax.random.fold_in(jax.random.fold_in(rng, 6), dim), (parts,), jnp.float32, least / len(pieces), largest / len(pieces))
        level = level * jnp.repeat(jnp.exp(heights), extent[dim] // parts).reshape((-1,) + (1,) * (len(extent) - 1 - dim))
    return level


def centred(own_key, dims, deviation, most, shards=(), kind=jnp.bfloat16):
    loudness = levels(own_key, dims, shards, -0.22, 0.18) if shards else 1.0
    entries = jax.random.normal(own_key, dims, jnp.float32) * deviation * loudness
    return jnp.minimum(jnp.maximum(entries, -most), most).astype(kind)


def setup_inputs(seed: int = 0) -> dict:
    splits = jax.random.split(jax.random.key(seed), 6)
    return {
        "inputs": centred(splits[0], (TOKENS, D), 1.0, 6.0, ((0, 4), (1, 4))),
        "upstream": centred(splits[1], (TOKENS, D), 1.0, 6.0, ((0, 4), (1, 4))),
        "expand": centred(splits[2], (D, FF), D ** -0.5, 0.09375, ((0, 4), (1, 2))),
        "biases": centred(splits[3], (FF,), 1.0, 5.0, ((0, 2),), jnp.float32),
        "contract": centred(splits[4], (FF, D), FF ** -0.5, 0.046875, ((0, 2), (1, 4))),
    }


def gelu_tanh(values):
    return jax.nn.gelu(values, approximate=True)

def rounded(values):
    return lax.optimization_barrier(values.astype(jnp.bfloat16)).astype(jnp.float32)

def reference(inputs, upstream, expand, biases, contract):
    width = D // N_ROW
    hidden_width = FF // N_COL
    pre_sum = jnp.zeros((TOKENS, FF), jnp.float32)
    back_sum = jnp.zeros((TOKENS, FF), jnp.float32)
    for index in range(N_ROW):
        first = index * width
        pre_part = jnp.dot(inputs[:, first:first + width], expand[first:first + width, :], preferred_element_type=jnp.float32)
        pre_sum = pre_sum + rounded(pre_part)
        back_part = jnp.dot(upstream[:, first:first + width], contract[:, first:first + width].T, preferred_element_type=jnp.float32)
        back_sum = back_sum + rounded(back_part)
    hidden = (pre_sum + biases[None, :]).astype(jnp.bfloat16)
    backward = back_sum.astype(jnp.bfloat16)
    forward_act, pullback = jax.vjp(gelu_tanh, hidden.astype(jnp.float32))
    slope_grad, = pullback(backward.astype(jnp.float32))
    activation = forward_act.astype(jnp.bfloat16)
    hidden_grad = slope_grad.astype(jnp.bfloat16)
    input_total = jnp.zeros((TOKENS, D), jnp.float32)
    for index in range(N_COL):
        first = index * hidden_width
        input_part = jnp.dot(hidden_grad[:, first:first + hidden_width], expand[:, first:first + hidden_width].T, preferred_element_type=jnp.float32)
        input_total = input_total + rounded(input_part)
    grad_inputs = input_total.astype(jnp.bfloat16)
    factor = TOKENS ** (-0.5)
    expand_total = jnp.zeros((D, FF), jnp.float32)
    biases_total = jnp.zeros((FF,), jnp.float32)
    contract_total = jnp.zeros((FF, D), jnp.float32)
    offset_total = jnp.zeros((D,), jnp.float32)
    for index in range(N_DP):
        first = index * TOK_DEV
        input_block = inputs[first:first + TOK_DEV]
        grad_block = hidden_grad[first:first + TOK_DEV]
        active_block = activation[first:first + TOK_DEV]
        upstream_block = upstream[first:first + TOK_DEV]
        expand_total = expand_total + rounded(jnp.dot(input_block.T, grad_block, preferred_element_type=jnp.float32) * factor)
        biases_total = biases_total + rounded(lax.optimization_barrier(jnp.sum(grad_block, axis=0, dtype=jnp.float32)) * factor)
        contract_total = contract_total + rounded(jnp.dot(active_block.T, upstream_block, preferred_element_type=jnp.float32) * factor)
        offset_total = offset_total + rounded(lax.optimization_barrier(jnp.sum(upstream_block, axis=0, dtype=jnp.float32)) * factor)
    return (grad_inputs, expand_total.astype(jnp.bfloat16), biases_total.astype(jnp.bfloat16), contract_total.astype(jnp.bfloat16), offset_total.astype(jnp.bfloat16))
```

```python
import jax
import jax.numpy as jnp
from jax import lax
from jax.sharding import PartitionSpec as P

F32 = jnp.float32
BF16 = jnp.bfloat16


def gelu_tanh(values):
    return jax.nn.gelu(values, approximate=True)


def add(a, b):
    return a.astype(F32) + b.astype(F32)


def dot(a, b, ca, cb):
    return lax.dot_general(a, b, (((ca,), (cb,)), ((), ())), preferred_element_type=F32)


def core_swap(x):
    return lax.ppermute(x, "dp", [(i, i ^ 1) for i in range(lax.axis_size("dp"))])


def far_swap(x):
    n = lax.axis_size("dp")
    return lax.ppermute(x, "dp", [(i, (i + n // 2) % n) for i in range(n)])


def col_swap(x):
    return lax.ppermute(x, "col", [(0, 1), (1, 0)])


def local(inputs, upstream, expand, biases, contract):
    n_row, n_col, n_dp = (lax.axis_size(a) for a in ("row", "col", "dp"))
    assert n_dp == 4
    row, col, dp = (lax.axis_index(a) for a in ("row", "col", "dp"))
    far, core = dp // 2, dp % 2
    tok, wid = inputs.shape
    hid = expand.shape[1]
    factor = (tok * n_dp) ** (-0.5)
    chunk = tok // n_col
    part = hid // (n_row * 4)

    def tokens(x):
        x = lax.dynamic_slice_in_dim(x, col * chunk, chunk, 0)
        x = lax.all_gather(x, "row", axis=1, tiled=True)
        if n_col == 2:
            x = jnp.concatenate([x, col_swap(x)], 0)
        else:
            x = lax.all_gather(x, "col", axis=0, tiled=True)
        return jnp.concatenate([x, core_swap(x)], 0)

    w1 = lax.dynamic_slice(
        expand.reshape(wid, n_row, 4, part), (0, 0, core * 2 + far, 0), (wid, n_row, 1, part)
    ).reshape(wid, n_row * part)
    w1 = lax.all_to_all(w1, "row", 1, 0, tiled=True)
    x_all = tokens(inputs)
    w1 = jnp.concatenate([w1, far_swap(w1)], 1)
    w2 = lax.dynamic_slice(
        contract.reshape(n_row, 4, part, wid), (0, core * 2 + far, 0, 0), (n_row, 1, part, wid)
    ).reshape(n_row * part, wid)
    u_all = tokens(upstream)
    w2 = lax.all_to_all(w2, "row", 0, 1, tiled=True)
    w2 = jnp.concatenate([w2, far_swap(w2)], 0)
    bias4 = biases.reshape(n_row, 4, part)
    bias = jnp.concatenate(
        [
            lax.dynamic_slice(bias4, (row, core * 2 + f, 0), (1, 1, part)).reshape(part)
            for f in (far, 1 - far)
        ]
    )

    hidden = (dot(x_all, w1, 1, 0) + bias[None, :]).astype(BF16).astype(F32)
    act, pullback = jax.vjp(gelu_tanh, hidden)
    act = act.astype(BF16)
    backward = dot(u_all, w2, 1, 1).astype(BF16)
    (grad,) = pullback(backward.astype(F32))
    grad = grad.astype(BF16)

    def home(own, far_part, split, concat):
        mine = add(own, far_swap(far_part.astype(BF16))).astype(BF16)
        mine = lax.all_to_all(mine, "row", split, concat, tiled=True)
        other = far_swap(mine)
        lo, hi = jnp.where(far == 0, mine, other), jnp.where(far == 0, other, mine)
        return lo, hi, core_swap(mine), core_swap(other)

    def four(own, far_part, split, concat):
        lo, hi, c_mine, c_other = home(own, far_part, split, concat)
        c_lo, c_hi = jnp.where(far == 0, c_mine, c_other), jnp.where(far == 0, c_other, c_mine)
        first = core == 0
        return (
            jnp.where(first, lo, c_lo),
            jnp.where(first, hi, c_hi),
            jnp.where(first, c_lo, lo),
            jnp.where(first, c_hi, hi),
        )

    c_far = dot(act[:, part:], u_all, 0, 0) * factor
    c_own = dot(act[:, :part], u_all, 0, 0) * factor
    pieces = four(c_own, c_far, 1, 0)
    grad_contract = jnp.stack([p.reshape(n_row, part, wid) for p in pieces], 1).reshape(hid, wid)

    e_far = dot(x_all, grad[:, part:], 0, 0) * factor
    e_own = dot(x_all, grad[:, :part], 0, 0) * factor
    pieces = four(e_own, e_far, 0, 1)
    grad_expand = jnp.stack([p.reshape(wid, n_row, part) for p in pieces], 2).reshape(wid, hid)

    g_far = dot(grad[tok:], w1, 1, 1).astype(BF16)
    g = add(dot(grad[:tok], w1, 1, 1), core_swap(g_far)).astype(BF16)
    if n_col == 2:
        g = add(g[:chunk], col_swap(g[chunk:])).astype(BF16)
    else:
        g = lax.psum_scatter(g, "col", scatter_dimension=0, tiled=True)
    g = lax.psum_scatter(g, "row", scatter_dimension=1, tiled=True)
    if n_col == 2:
        other = col_swap(g)
        first = col == 0
        grad_inputs = jnp.concatenate(
            [jnp.where(first, g, other), jnp.where(first, other, g)], 0
        )
    else:
        grad_inputs = lax.all_gather(g, "col", axis=0, tiled=True)

    b_sum = jnp.sum(grad, axis=0, dtype=F32) * factor
    b_all = jnp.zeros((n_row, 4, part), F32)
    for i, f in enumerate((far, 1 - far)):
        b_all = lax.dynamic_update_slice(
            b_all, b_sum[i * part : (i + 1) * part].reshape(1, 1, part), (row, core * 2 + f, 0)
        )
    o_sum = jnp.sum(upstream, axis=0, dtype=F32) * factor
    o_all = lax.dynamic_update_slice(jnp.zeros((n_row, wid), F32), o_sum[None], (row, 0))
    small = lax.psum(jnp.concatenate([b_all.reshape(-1), o_all.reshape(-1)]), ("row", "dp"))
    grad_biases = small[:hid].astype(BF16)
    grad_offset = lax.dynamic_slice_in_dim(small[hid:], row * wid, wid).astype(BF16)
    return grad_inputs, grad_expand, grad_biases, grad_contract, grad_offset


def solution(mesh):
    in_specs = (P("dp", "row"), P("dp", "row"), P("row", "col"), P("col"), P("col", "row"))
    out_specs = (P("dp", "row"), P("row", "col"), P("col"), P("col", "row"), P("row"))
    return jax.shard_map(local, mesh=mesh, in_specs=in_specs, out_specs=out_specs, check_vma=False)
```
